32 devices in a mesh: group: 2 (over x), feat: 16 (over z, y, core).
Axes of the slice: x: 2, y: 2, z: 4, core: 2. Of those that a mesh axis runs over, the one named last changes fastest.
Arguments:
- store_inputs: bfloat16 [2, 512, 2048], P(None, ('group', 'feat')), parts along dimension 1, may hold values from -6 to 6
- store_targets: bfloat16 [2, 512, 2048], P(None, ('group', 'feat')), parts along dimension 1, may hold values from -6 to 6
- row_ids: int32 [256], P(('group', 'feat')), parts along dimension 0, may hold values from 0 to 15
- enc_weight: bfloat16 [2, 2048, 16384], P(None, None, 'feat'), may hold values from -0.125 to 0.125
- enc_bias: float32 [2, 16384], P(None, 'feat'), may hold values from -3 to 3
- dec_weight: bfloat16 [3, 16384, 2048], P(None, 'feat'), may hold values from -0.046875 to 0.046875
Outputs:
- enc_grad: bfloat16 [4, 2048, 16384], P('group', None, 'feat'), parts along dimension 0
- bias_grad: float32 [4, 16384], P('group', 'feat'), parts along dimension 0
- dec_grad: bfloat16 [6, 16384, 2048], P('group', 'feat'), parts along dimension 0
The draws below stay inside these ranges and needn't reach their ends.
There are 2 independent parts, one for each index of `group`. The reference program is written for one: setup_inputs(seed, part) draws one part's arguments, and reference() takes and returns one part's arrays. A program takes and returns all parts, laid end to end along the dimension named above; an argument that names none is the same for every part. Nothing has to cross between parts.
Inputs may be any that keep to these rules, and one draw needn't show every extreme that they name: row_ids[i] indexes the store rows held with token i, as in the first step.
All inputs are finite; a program needn't handle non-finite values.
Results may differ from the reference program's by a relative error of at most 0.035.
Values may be sent and summed in bfloat16 or wider, within the bound.
No kernel may reach another device: no remote copies, remote signals or barrier semaphores. Data moves between devices by JAX's collectives and lax.ppermute only.
A program may use at most 128 MiB of HBM per device.

```python
import math
import jax
import jax.numpy as jnp
from jax import lax

D = 2048
F = 16384
L = 2
TOK_DEV = 8
PAIRS = 3
BUF_DEV = 16
TOKENS = 128
BUF = 256


def plant(array, rng, least, largest):
    place = [jax.random.randint(jax.random.fold_in(rng, axis), (), 0, length) for axis, length in enumerate(array.shape)]
    widest = array.shape.index(max(array.shape))
    beside = place[:widest] + [(place[widest] + 1) % array.shape[widest]] + place[widest + 1:]
    return array.at[tuple(place)].set(least).at[tuple(beside)].set(largest)


def level_of(stream_key, dims, pieces, smallest, largest):
    gain = 1.0
    for axis_at, blocks in pieces:
        heights = jax.random.uniform(jax.random.fold_in(jax.random.fold_in(stream_key, 6), axis_at), (blocks,), jnp.float32, smallest / len(pieces), largest / len(pieces))
        gain = gain * jnp.repeat(jnp.exp(heights), dims[axis_at] // blocks).reshape((-1,) + (1,) * (len(dims) - 1 - axis_at))
    return gain


def normal_values(rng, dims, deviation, reach, split=(), held_as=jnp.bfloat16):
    array = deviation * jax.random.normal(rng, dims, jnp.float32)
    if split:
        array = array * level_of(rng, dims, split, -0.22, 0.18)
    return jnp.clip(array, -reach, reach).astype(held_as)


def setup_inputs(seed: int = 0, part: int = 0) -> dict:
    splits = jax.random.split(jax.random.key(seed), 7)
    part_keys = jax.random.split(jax.random.fold_in(splits[6], part), 7)
    return {
        "store_inputs": normal_values(part_keys[0], (L, BUF, D), 1.0, 6.0, ((1, 16),)),
        "store_targets": normal_values(part_keys[1], (L, BUF, D), 1.0, 6.0, ((1, 16),)),
        "row_ids": plant(jax.random.randint(part_keys[2], (TOKENS,), 0, BUF_DEV), jax.random.fold_in(part_keys[2], 1), 0, BUF_DEV - 1).astype(jnp.int32),
        "enc_weight": normal_values(splits[3], (L, D, F), D ** -0.5, 0.125, ((2, 16),)),
        "enc_bias": normal_values(splits[4], (L, F), 0.5, 3.0, ((1, 16),), jnp.float32),
        "dec_weight": normal_values(splits[5], (PAIRS, F, D), F ** -0.5, 0.046875, ((1, 16),)),
    }


def reference(store_inputs, store_targets, row_ids, enc_weight, enc_bias, dec_weight):
    row_index = jnp.arange(TOKENS, dtype=jnp.int32) // TOK_DEV * BUF_DEV + row_ids.astype(jnp.int32)
    inputs = jnp.take(store_inputs, row_index, axis=1)
    targets = jnp.take(store_targets, row_index, axis=1)
    grad_scale = 1.0 / math.sqrt(TOKENS)
    pair_list = [(source, target) for source in range(L) for target in range(source, L)]
    preact = [jnp.dot(inputs[index], enc_weight[index], preferred_element_type=jnp.float32) + enc_bias[index] for index in range(L)]
    features = [jnp.maximum(value, 0.0).astype(jnp.bfloat16) for value in preact]
    errors = []
    for target in range(L):
        rebuilt = jnp.zeros((TOKENS, D), jnp.float32)
        for index, (source, goal) in enumerate(pair_list):
            if goal == target:
                rebuilt = rebuilt + jnp.dot(features[source], dec_weight[index], preferred_element_type=jnp.float32)
        errors.append((rebuilt - targets[target].astype(jnp.float32)).astype(jnp.bfloat16))
    dec_list = []
    feature_grad = [jnp.zeros((TOKENS, F), jnp.float32) for index in range(L)]
    for index, (source, target) in enumerate(pair_list):
        product = jnp.dot(features[source].T, errors[target], preferred_element_type=jnp.float32)
        dec_list.append((grad_scale * product).astype(jnp.bfloat16))
        feature_grad[source] = feature_grad[source] + lax.dot_general(errors[target], dec_weight[index], (((1,), (1,)), ((), ())), preferred_element_type=jnp.float32)
    enc_list = []
    bias_list = []
    for index in range(L):
        pre_grad = jnp.where(preact[index] > 0, feature_grad[index], 0.0) * grad_scale
        bias_list.append(lax.optimization_barrier(jnp.sum(pre_grad, axis=0)))
        enc_list.append(jnp.dot(inputs[index].T, pre_grad.astype(jnp.bfloat16), preferred_element_type=jnp.float32).astype(jnp.bfloat16))
    return (jnp.stack(enc_list), jnp.stack(bias_list), jnp.stack(dec_list))
```

```python
import math

import jax
import jax.numpy as jnp
from jax import lax
from jax.sharding import PartitionSpec as P


def swap(value, mask, size):
    return lax.ppermute(value, "feat", [(index, index ^ mask) for index in range(size)])


def gather_rows(own, size):
    if size == 1:
        return own
    rows = own.shape[0]
    slots = {0: own}
    far = [4 * step for step in range(1, size // 4)]
    for mask in far[::-1]:
        slots[mask] = swap(own, mask, size)
    if size > 2:
        slots[2] = swap(own, 2, size)
        if far:
            block = swap(jnp.concatenate([slots[mask] for mask in far], axis=0), 2, size)
            for index, mask in enumerate(far):
                slots[mask + 2] = block[index * rows : (index + 1) * rows]
    even = jnp.concatenate([slots[mask] for mask in range(0, size, 2)], axis=0)
    odd = swap(even, 1, size)
    return even, odd


def scatter_sums(parts, size):
    got = swap(parts[:, 1], 1, size)
    pair = (parts[:, 0].astype(jnp.float32) + got.astype(jnp.float32)).astype(jnp.bfloat16)
    total = pair[0].astype(jnp.float32)
    for slot in range(1, size // 2):
        total = total + swap(pair[slot], 2 * slot, size).astype(jnp.float32)
    return total


def local(store_inputs, store_targets, row_ids, enc_weight, enc_bias, dec_weight):
    size = lax.axis_size("feat")
    layers, width, tile = enc_weight.shape
    rows = row_ids.shape[0]
    pairs = [(source, target) for source in range(layers) for target in range(source, layers)]
    tokens = rows * size
    grad_scale = 1.0 / math.sqrt(tokens)

    picked_in = jnp.take(store_inputs, row_ids, axis=1).transpose(1, 0, 2).reshape(rows, layers * width)
    picked_out = jnp.take(store_targets, row_ids, axis=1).transpose(1, 0, 2).reshape(rows, layers * width)

    even, odd = gather_rows(picked_in, size)
    inputs = jnp.concatenate([even, odd], axis=0).reshape(tokens, layers, width).transpose(1, 0, 2)
    preact = [
        jnp.dot(inputs[layer], enc_weight[layer], preferred_element_type=jnp.float32) + enc_bias[layer]
        for layer in range(layers)
    ]
    features = [jnp.maximum(value, 0.0).astype(jnp.bfloat16) for value in preact]
    rebuilt = []
    for target in range(layers):
        total = jnp.zeros((tokens, width), jnp.float32)
        for index, (source, goal) in enumerate(pairs):
            if goal == target:
                total = total + jnp.dot(
                    features[source], dec_weight[index], preferred_element_type=jnp.float32
                )
        rebuilt.append(total.astype(jnp.bfloat16))
    parts = jnp.concatenate(rebuilt, axis=1).reshape(2, size // 2, rows, layers * width)
    own = scatter_sums(parts.transpose(1, 0, 2, 3), size)
    errors_own = (own - picked_out.astype(jnp.float32)).astype(jnp.bfloat16)
    even, odd = gather_rows(errors_own, size)
    errors = jnp.concatenate([even, odd], axis=0).reshape(tokens, layers, width).transpose(1, 0, 2)

    pair_features = jnp.stack([features[source] for source, _ in pairs])
    pair_errors = jnp.stack([errors[target] for _, target in pairs])
    dec_grad = (
        grad_scale
        * jnp.einsum("pbf,pbd->pfd", pair_features, pair_errors, preferred_element_type=jnp.float32)
    ).astype(jnp.bfloat16)
    feature_grad = [jnp.zeros((tokens, tile), jnp.float32) for _ in range(layers)]
    for index, (source, target) in enumerate(pairs):
        feature_grad[source] = feature_grad[source] + lax.dot_general(
            errors[target], dec_weight[index], (((1,), (1,)), ((), ())), preferred_element_type=jnp.float32
        )
    pre_grad = jnp.stack(
        [jnp.where(preact[layer] > 0, feature_grad[layer], 0.0) * grad_scale for layer in range(layers)]
    )
    bias_grad = jnp.sum(pre_grad, axis=1)
    enc_grad = jnp.einsum(
        "lbd,lbf->ldf", inputs, pre_grad.astype(jnp.bfloat16), preferred_element_type=jnp.float32
    ).astype(jnp.bfloat16)
    return (enc_grad, bias_grad, dec_grad)


def solution(mesh):
    in_specs = (
        P(None, ("group", "feat"), None),
        P(None, ("group", "feat"), None),
        P(("group", "feat")),
        P(None, None, "feat"),
        P(None, "feat"),
        P(None, "feat", None),
    )
    out_specs = (P("group", None, "feat"), P("group", "feat"), P("group", "feat", None))
    return jax.shard_map(local, mesh=mesh, in_specs=in_specs, out_specs=out_specs, check_vma=False)
```

```python
import functools
import math

import jax
import jax.numpy as jnp
from jax import lax
from jax.experimental import pallas as pl
from jax.experimental.pallas import tpu as pltpu
from jax.sharding import PartitionSpec as P

MIB = 1 << 20
SLOTS = 6
WHOLE = pl.BlockSpec(memory_space=pltpu.VMEM)
HELD = pl.BlockSpec(memory_space=pl.ANY)


def pair_list(layers):
    return [(source, target) for source in range(layers) for target in range(source, layers)]


def params(limit):
    return pltpu.CompilerParams(vmem_limit_bytes=limit)


def cost(flops, moved):
    return pl.CostEstimate(flops=int(flops), transcendentals=0, bytes_accessed=int(moved))


def in_vmem(array):
    return pltpu.with_memory_space_constraint(array, pltpu.VMEM)


def swap(value, mask, size):
    return lax.ppermute(value, "feat", [(index, index ^ mask) for index in range(size)])


def slot_order(size):
    if size < 4:
        return [0]
    far = list(range(0, size, 4))
    return far + [mask + 2 for mask in far]


def gather_rows(own, size):
    if size == 1:
        return own, None
    if size == 2:
        return own, swap(own, 1, size)
    far = [4 * step for step in range(1, size // 4)]
    got = {mask: swap(own, mask, size) for mask in far[::-1]}
    parts = [own] + [got[mask] for mask in far] + [swap(own, 2, size)]
    if far:
        parts.append(swap(jnp.concatenate([got[mask] for mask in far], axis=0), 2, size))
    even = jnp.concatenate(parts, axis=0)
    return even, swap(even, 1, size)


def scatter_sums(keep, send, size, rows):
    got = swap(send, 1, size)
    pair = (keep.astype(jnp.float32) + got.astype(jnp.float32)).astype(jnp.bfloat16)
    total = pair[:rows].astype(jnp.float32)
    for slot, mask in enumerate(slot_order(size)):
        if mask:
            total = total + swap(pair[slot * rows : (slot + 1) * rows], mask, size).astype(jnp.float32)
    return total


def pick_kernel(ids_ref, in_ref, out_ref, picked_in, picked_out):
    layers, buf, width = in_ref.shape
    rows = ids_ref.shape[0]
    place = lax.broadcasted_iota(jnp.int32, (rows, buf), 0)
    wanted = jnp.zeros((rows, buf), jnp.int32)
    for row in range(rows):
        wanted = jnp.where(place == row, ids_ref[row], wanted)
    hot = jnp.where(wanted == lax.broadcasted_iota(jnp.int32, (rows, buf), 1), 1.0, 0.0).astype(jnp.bfloat16)
    for layer in range(layers):
        columns = slice(layer * width, (layer + 1) * width)
        picked_in[:, columns] = jnp.dot(hot, in_ref[layer], preferred_element_type=jnp.float32).astype(
            jnp.bfloat16
        )
        picked_out[:, columns] = jnp.dot(hot, out_ref[layer], preferred_element_type=jnp.float32).astype(
            jnp.bfloat16
        )


def pick(row_ids, store_inputs, store_targets):
    layers, _, width = store_inputs.shape
    shape = jax.ShapeDtypeStruct((row_ids.shape[0], layers * width), jnp.bfloat16)
    return pl.pallas_call(
        pick_kernel,
        out_shape=(shape, shape),
        in_specs=[pl.BlockSpec(memory_space=pltpu.SMEM), WHOLE, WHOLE],
        out_specs=[WHOLE, WHOLE],
        compiler_params=params(4 * MIB),
        name="pick",
    )(row_ids, store_inputs, store_targets)


def load_kernel(enc_ref, dec_ref, enc_out, dec_out, sems):
    copies = [
        pltpu.make_async_copy(enc_ref.at[layer], enc_out.at[layer], sems.at[layer])
        for layer in range(enc_ref.shape[0])
    ]
    copies += [
        pltpu.make_async_copy(dec_ref.at[index], dec_out.at[index], sems.at[len(copies) + index])
        for index in range(dec_ref.shape[0])
    ]
    for copy in copies:
        copy.start()
    for copy in copies:
        copy.wait()


def load_weights(enc_weight, dec_weight):
    moved = 4 * (enc_weight.size + dec_weight.size)
    return pl.pallas_call(
        load_kernel,
        out_shape=(
            pltpu.VMEM(enc_weight.shape, enc_weight.dtype),
            pltpu.VMEM(dec_weight.shape, dec_weight.dtype),
        ),
        in_specs=[HELD, HELD],
        out_specs=[WHOLE, WHOLE],
        scratch_shapes=[pltpu.SemaphoreType.DMA((enc_weight.shape[0] + dec_weight.shape[0],))],
        compiler_params=params(2 * MIB),
        cost_estimate=cost(moved * 100, moved),
        name="load_weights",
    )(
        pltpu.with_memory_space_constraint(enc_weight, pltpu.HBM),
        pltpu.with_memory_space_constraint(dec_weight, pltpu.HBM),
    )


def forward_kernel(even_ref, odd_ref, enc_ref, bias_ref, dec_ref, keep_ref, send_ref, feat_ref, x_ref):
    layers, width, tile = enc_ref.shape
    half = even_ref.shape[0]
    x_ref[:half] = even_ref[...]
    x_ref[half:] = odd_ref[...]
    chunk = min(256, tile)
    for layer in range(layers):

        @pl.loop(0, tile // chunk)
        def _(step):
            columns = pl.ds(pl.multiple_of(step * chunk, chunk), chunk)
            value = jnp.dot(
                x_ref[:, layer * width : (layer + 1) * width],
                enc_ref[layer, :, columns],
                preferred_element_type=jnp.float32,
            )
            value = value + bias_ref[layer : layer + 1, columns]
            feat_ref[layer, :, columns] = jnp.maximum(value, 0.0).astype(jnp.bfloat16)

    span = min(512, width)
    for target in range(layers):

        @pl.loop(0, width // span)
        def _(step):
            columns = pl.ds(pl.multiple_of(step * span, span), span)
            total = None
            for index, (source, goal) in enumerate(pair_list(layers)):
                if goal == target:
                    term = jnp.dot(
                        feat_ref[source], dec_ref[index, :, columns], preferred_element_type=jnp.float32
                    )
                    total = term if total is None else total + term
            total = total.astype(jnp.bfloat16)
            places = pl.ds(pl.multiple_of(target * width + step * span, span), span)
            keep_ref[:, places] = total[:half]
            send_ref[:, places] = total[half:]


def forward(even, odd, enc_weight, enc_bias, dec_weight):
    layers, width, tile = enc_weight.shape
    half, wide = even.shape
    side = jax.ShapeDtypeStruct((half, wide), jnp.bfloat16)
    return pl.pallas_call(
        forward_kernel,
        out_shape=(
            side,
            side,
            jax.ShapeDtypeStruct((layers, 2 * half, tile), jnp.bfloat16),
            jax.ShapeDtypeStruct((2 * half, wide), jnp.bfloat16),
        ),
        in_specs=[WHOLE] * 5,
        out_specs=[WHOLE] * 4,
        compiler_params=params(16 * MIB),
        cost_estimate=cost(4 * half * (enc_weight.size + dec_weight.size), 0),
        name="forward",
    )(even, odd, in_vmem(enc_weight), enc_bias, in_vmem(dec_weight))


def turn_kernel(x_ref, feat_ref, x_out, feat_out):
    x_out[...] = x_ref[...].T
    for layer in range(feat_ref.shape[0]):
        feat_out[layer] = feat_ref[layer].T


def turn(x, feats):
    layers, tokens, tile = feats.shape
    return pl.pallas_call(
        turn_kernel,
        out_shape=(
            jax.ShapeDtypeStruct((x.shape[1], tokens), jnp.bfloat16),
            jax.ShapeDtypeStruct((layers, tile, tokens), jnp.bfloat16),
        ),
        in_specs=[WHOLE] * 2,
        out_specs=[WHOLE] * 2,
        compiler_params=params(16 * MIB),
        cost_estimate=cost(2000 * (x.size + feats.size), 0),
        name="turn",
    )(x, feats)


def backward_kernel(
    scale,
    even_ref,
    odd_ref,
    feat_ref,
    feat_t_ref,
    x_t_ref,
    dec_ref,
    enc_out,
    bias_out,
    dec_out,
    e_ref,
    pre_ref,
    stage_dec,
    stage_enc,
    sems_dec,
    sems_enc,
):
    pairs, tile, width = dec_ref.shape
    layers = feat_ref.shape[0]
    half = even_ref.shape[0]
    e_ref[:half] = even_ref[...]
    e_ref[half:] = odd_ref[...]
    chunk = stage_dec.shape[1]
    steps = tile // chunk

    def dec_copy(index, step, slot):
        rows = pl.ds(pl.multiple_of(step * chunk, chunk), chunk)
        return pltpu.make_async_copy(stage_dec.at[slot], dec_out.at[index, rows], sems_dec.at[slot])

    for index, (source, target) in enumerate(pair_list(layers)):

        @pl.loop(0, steps)
        def _(step):
            slot = lax.rem(index * steps + step, SLOTS)

            @pl.when(index * steps + step >= SLOTS)
            def _():
                dec_copy(index, step, slot).wait()

            rows = pl.ds(pl.multiple_of(step * chunk, chunk), chunk)
            value = jnp.dot(
                feat_t_ref[source, rows, :],
                e_ref[:, target * width : (target + 1) * width],
                preferred_element_type=jnp.float32,
            )
            stage_dec[slot] = (scale * value).astype(jnp.bfloat16)
            dec_copy(index, step, slot).start()

    for layer in range(layers):

        @pl.loop(0, steps)
        def _(step):
            columns = pl.ds(pl.multiple_of(step * chunk, chunk), chunk)
            total = None
            for index, (source, target) in enumerate(pair_list(layers)):
                if source == layer:
                    term = lax.dot_general(
                        e_ref[:, target * width : (target + 1) * width],
                        dec_ref[index, columns, :],
                        (((1,), (1,)), ((), ())),
                        preferred_element_type=jnp.float32,
                    )
                    total = term if total is None else total + term
            pre = jnp.where(feat_ref[layer, :, columns] > 0, total, 0.0) * scale
            bias_out[layer : layer + 1, columns] = jnp.sum(pre, axis=0, keepdims=True)
            pre_ref[layer, :, columns] = pre.astype(jnp.bfloat16)

    span = stage_enc.shape[1]
    enc_steps = width // span

    def enc_copy(layer, step, slot):
        rows = pl.ds(pl.multiple_of(step * span, span), span)
        return pltpu.make_async_copy(stage_enc.at[slot], enc_out.at[layer, rows], sems_enc.at[slot])

    for layer in range(layers):

        @pl.loop(0, enc_steps)
        def _(step):
            slot = lax.rem(layer * enc_steps + step, SLOTS)

            @pl.when(layer * enc_steps + step >= SLOTS)
            def _():
                enc_copy(layer, step, slot).wait()

            rows = pl.ds(pl.multiple_of(layer * width + step * span, span), span)
            value = jnp.dot(x_t_ref[rows, :], pre_ref[layer], preferred_element_type=jnp.float32)
            stage_enc[slot] = value.astype(jnp.bfloat16)
            enc_copy(layer, step, slot).start()

    for slot in range(min(SLOTS, pairs * steps)):
        dec_copy(0, 0, slot).wait()
    for slot in range(min(SLOTS, layers * enc_steps)):
        enc_copy(0, 0, slot).wait()


def backward(scale, even, odd, feats, feats_t, x_t, dec_weight):
    layers, tokens, tile = feats.shape
    pairs, _, width = dec_weight.shape
    chunk = min(256, tile)
    span = min(512, width)
    return pl.pallas_call(
        functools.partial(backward_kernel, scale),
        out_shape=(
            jax.ShapeDtypeStruct((layers, width, tile), jnp.bfloat16),
            jax.ShapeDtypeStruct((layers, tile), jnp.float32),
            jax.ShapeDtypeStruct((pairs, tile, width), jnp.bfloat16),
        ),
        in_specs=[WHOLE] * 6,
        out_specs=[HELD, WHOLE, HELD],
        scratch_shapes=[
            pltpu.VMEM((tokens, layers * width), jnp.bfloat16),
            pltpu.VMEM((layers, tokens, tile), jnp.bfloat16),
            pltpu.VMEM((SLOTS, chunk, width), jnp.bfloat16),
            pltpu.VMEM((SLOTS, span, tile), jnp.bfloat16),
            pltpu.SemaphoreType.DMA((SLOTS,)),
            pltpu.SemaphoreType.DMA((SLOTS,)),
        ],
        compiler_params=params(28 * MIB),
        cost_estimate=cost(10 * tokens * dec_weight.size, 0),
        name="backward",
    )(even, odd, feats, feats_t, x_t, in_vmem(dec_weight))


def local(store_inputs, store_targets, row_ids, enc_weight, enc_bias, dec_weight):
    size = lax.axis_size("feat")
    rows = row_ids.shape[0]
    scale = 1.0 / math.sqrt(rows * size)
    picked_in, picked_out = pick(row_ids, store_inputs, store_targets)
    enc_near, dec_near = load_weights(enc_weight, dec_weight)
    even, odd = gather_rows(picked_in, size)
    keep, send, feats, x = forward(even, odd, enc_near, enc_bias, dec_near)
    x_t, feats_t = turn(x, feats)
    own = scatter_sums(keep, send, size, rows)
    errors_own = (own - picked_out.astype(jnp.float32)).astype(jnp.bfloat16)
    even, odd = gather_rows(errors_own, size)
    return backward(scale, even, odd, feats, feats_t, x_t, dec_near)


def solution(mesh):
    in_specs = (
        P(None, ("group", "feat"), None),
        P(None, ("group", "feat"), None),
        P(("group", "feat")),
        P(None, None, "feat"),
        P(None, "feat"),
        P(None, "feat", None),
    )
    out_specs = (P("group", None, "feat"), P("group", "feat"), P("group", "feat", None))
    return jax.shard_map(local, mesh=mesh, in_specs=in_specs, out_specs=out_specs, check_vma=False)
```

```python
import functools
import math

import jax
import jax.numpy as jnp
from jax import lax
from jax.experimental import pallas as pl
from jax.experimental.pallas import tpu as pltpu
from jax.sharding import PartitionSpec as P

MIB = 1 << 20
WHOLE = pl.BlockSpec(memory_space=pltpu.VMEM)
HELD = pl.BlockSpec(memory_space=pl.ANY)


def pair_list(layers):
    return [(source, target) for source in range(layers) for target in range(source, layers)]


def params(limit):
    return pltpu.CompilerParams(vmem_limit_bytes=limit)


def cost(flops, moved):
    return pl.CostEstimate(flops=int(flops), transcendentals=0, bytes_accessed=int(moved))


def in_vmem(array):
    return pltpu.with_memory_space_constraint(array, pltpu.VMEM)


def swap(value, mask, size):
    return lax.ppermute(value, "feat", [(index, index ^ mask) for index in range(size)])


def slot_order(size):
    if size < 4:
        return [0]
    far = list(range(0, size, 4))
    return far + [mask + 2 for mask in far]


def gather_rows(own, size, beside=(), later=None):
    if size < 8:
        even = own if size == 2 else jnp.concatenate([own, swap(own, 2, size)], axis=0)
        return [even, swap(even, 1, size)], beside, later(()) if later else None
    far = [4 * step for step in range(1, size // 4)]
    got = {mask: swap(own, mask, size) for mask in far}
    side = swap(own, 2, size)
    late = [swap(got[far[0]], 2, size)]
    rest, beside = lax.optimization_barrier(([got[mask] for mask in far[1:]], beside))
    late.append(swap(jnp.concatenate(rest, axis=0), 2, size))
    early = jnp.concatenate([own, got[far[0]]] + rest + [side], axis=0)
    early_pair = swap(early, 1, size)
    late = jnp.concatenate(late, axis=0)
    made = None
    if later:
        late, made = lax.optimization_barrier((late, later(rest[:1])))
    return [early, late, early_pair, swap(late, 1, size)], beside, made


def scatter_sums(keep, send, size, rows):
    got = swap(send, 1, size)
    pair = (keep.astype(jnp.float32) + got.astype(jnp.float32)).astype(jnp.bfloat16)
    total = pair[:rows].astype(jnp.float32)
    for slot, mask in enumerate(slot_order(size)):
        if mask:
            total = total + swap(pair[slot * rows : (slot + 1) * rows], mask, size).astype(jnp.float32)
    return total


def pick_kernel(ids_hbm, in_hbm, out_hbm, picked_in, picked_out, ids_ref, in_ref, out_ref, sems):
    layers, buf, width = in_ref.shape
    rows = ids_ref.shape[0]
    copies = [
        pltpu.make_async_copy(ids_hbm, ids_ref, sems.at[0]),
        pltpu.make_async_copy(in_hbm, in_ref, sems.at[1]),
        pltpu.make_async_copy(out_hbm, out_ref, sems.at[2]),
    ]
    for copy in copies:
        copy.start()
    for copy in copies:
        copy.wait()
    place = lax.broadcasted_iota(jnp.int32, (rows, buf), 0)
    wanted = jnp.zeros((rows, buf), jnp.int32)
    for row in range(rows):
        wanted = jnp.where(place == row, ids_ref[row], wanted)
    hot = jnp.where(wanted == lax.broadcasted_iota(jnp.int32, (rows, buf), 1), 1.0, 0.0).astype(jnp.bfloat16)
    for layer in range(layers):
        columns = slice(layer * width, (layer + 1) * width)
        for ref, picked in ((in_ref, picked_in), (out_ref, picked_out)):
            picked[:, columns] = jnp.dot(hot, ref[layer], preferred_element_type=jnp.float32).astype(jnp.bfloat16)


def pick(row_ids, store_inputs, store_targets):
    layers, _, width = store_inputs.shape
    shape = jax.ShapeDtypeStruct((row_ids.shape[0], layers * width), jnp.bfloat16)
    return pl.pallas_call(
        pick_kernel,
        out_shape=(shape, shape),
        in_specs=[HELD] * 3,
        out_specs=[WHOLE, WHOLE],
        scratch_shapes=[
            pltpu.SMEM(row_ids.shape, jnp.int32),
            pltpu.VMEM(store_inputs.shape, jnp.bfloat16),
            pltpu.VMEM(store_targets.shape, jnp.bfloat16),
            pltpu.SemaphoreType.DMA((3,)),
        ],
        compiler_params=params(4 * MIB),
        name="pick",
    )(*(pltpu.with_memory_space_constraint(array, pltpu.HBM) for array in (row_ids, store_inputs, store_targets)))


def load_kernel(ref, *refs):
    out, sems = refs[-2:]
    copies = [
        pltpu.make_async_copy(ref.at[index], out.at[index], sems.at[index]) for index in range(ref.shape[0])
    ]
    for copy in copies:
        copy.start()
    for copy in copies:
        copy.wait()


def load(weight, after=()):
    moved = 4 * weight.size
    return pl.pallas_call(
        load_kernel,
        out_shape=pltpu.VMEM(weight.shape, weight.dtype),
        in_specs=[HELD] * (1 + len(after)),
        out_specs=WHOLE,
        scratch_shapes=[pltpu.SemaphoreType.DMA((weight.shape[0],))],
        compiler_params=params(2 * MIB),
        cost_estimate=cost(moved * 100, moved),
        name="load",
    )(pltpu.with_memory_space_constraint(weight, pltpu.HBM), *after)


def join(part_refs, out_ref):
    start = 0
    for ref in part_refs:
        out_ref[start : start + ref.shape[0]] = ref[...]
        start += ref.shape[0]


def forward_kernel(*refs):
    enc_ref, bias_ref, dec_ref, keep_ref, send_ref, feat_ref, x_ref = refs[-7:]
    layers, width, tile = enc_ref.shape
    half = keep_ref.shape[0]
    join(refs[:-7], x_ref)
    chunk = min(256, tile)
    for layer in range(layers):

        for step in range(tile // chunk):
            columns = pl.ds(step * chunk, chunk)
            value = jnp.dot(
                x_ref[:, layer * width : (layer + 1) * width],
                enc_ref[layer, :, columns],
                preferred_element_type=jnp.float32,
            )
            value = value + bias_ref[layer : layer + 1, columns]
            feat_ref[layer, :, columns] = jnp.maximum(value, 0.0).astype(jnp.bfloat16)

    span = min(512, width)
    for target in range(layers):

        for step in range(width // span):
            columns = pl.ds(step * span, span)
            total = None
            for index, (source, goal) in enumerate(pair_list(layers)):
                if goal == target:
                    term = jnp.dot(
                        feat_ref[source], dec_ref[index, :, columns], preferred_element_type=jnp.float32
                    )
                    total = term if total is None else total + term
            total = total.astype(jnp.bfloat16)
            places = pl.ds(target * width + step * span, span)
            keep_ref[:, places] = total[:half]
            send_ref[:, places] = total[half:]


def forward(parts, enc_weight, enc_bias, dec_weight):
    layers, width, tile = enc_weight.shape
    half, wide = sum(part.shape[0] for part in parts) // 2, parts[0].shape[1]
    side = jax.ShapeDtypeStruct((half, wide), jnp.bfloat16)
    return pl.pallas_call(
        forward_kernel,
        out_shape=(
            side,
            side,
            jax.ShapeDtypeStruct((layers, 2 * half, tile), jnp.bfloat16),
            jax.ShapeDtypeStruct((2 * half, wide), jnp.bfloat16),
        ),
        in_specs=[WHOLE] * (len(parts) + 3),
        out_specs=[WHOLE] * 4,
        compiler_params=params(16 * MIB),
        cost_estimate=cost(4 * half * (enc_weight.size + dec_weight.size), 0),
        name="forward",
    )(*parts, in_vmem(enc_weight), enc_bias, in_vmem(dec_weight))


def turn_kernel(x_ref, feat_ref, x_out, feat_out):
    x_out[...] = x_ref[...].T
    for layer in range(feat_ref.shape[0]):
        feat_out[layer] = feat_ref[layer].T


def turn(x, feats):
    layers, tokens, tile = feats.shape
    return pl.pallas_call(
        turn_kernel,
        out_shape=(
            jax.ShapeDtypeStruct((x.shape[1], tokens), jnp.bfloat16),
            jax.ShapeDtypeStruct((layers, tile, tokens), jnp.bfloat16),
        ),
        in_specs=[WHOLE] * 2,
        out_specs=[WHOLE] * 2,
        compiler_params=params(16 * MIB),
        cost_estimate=cost(2000 * (x.size + feats.size), 0),
        name="turn",
    )(x, feats)


def backward_kernel(scale, *refs):
    parts, refs = refs[:-13], refs[-13:]
    feat_ref, feat_t_ref, x_t_ref, dec_ref, enc_out, bias_out, dec_out = refs[:7]
    e_ref, pre_ref, stage_dec, stage_enc, dec_sem, enc_sem = refs[7:]
    pairs, tile, width = dec_ref.shape
    layers = feat_ref.shape[0]
    pair_of = pair_list(layers)
    join(parts, e_ref)
    chunk = min(256, tile)
    span = min(512, width)

    def dec_step(index, step):
        source, target = pair_of[index]
        place = pl.ds(step * chunk, chunk)
        value = jnp.dot(
            feat_t_ref[source, place, :],
            e_ref[:, target * width : (target + 1) * width],
            preferred_element_type=jnp.float32,
        )
        stage_dec[index, place, :] = (scale * value).astype(jnp.bfloat16)
        pltpu.make_async_copy(stage_dec.at[index, place], dec_out.at[index, place], dec_sem).start()

    def pre_step(layer, step):
        place = pl.ds(step * chunk, chunk)
        total = None
        for index, (source, target) in enumerate(pair_of):
            if source == layer:
                term = lax.dot_general(
                    e_ref[:, target * width : (target + 1) * width],
                    dec_ref[index, place, :],
                    (((1,), (1,)), ((), ())),
                    preferred_element_type=jnp.float32,
                )
                total = term if total is None else total + term
        pre = jnp.where(feat_ref[layer, :, place] > 0, total, 0.0) * scale
        bias_out[layer : layer + 1, place] = jnp.sum(pre, axis=0, keepdims=True)
        pre_ref[layer, :, place] = pre.astype(jnp.bfloat16)

    def enc_step(layer, step):
        place = pl.ds(step * span, span)
        rows = pl.ds(layer * width + step * span, span)
        value = jnp.dot(x_t_ref[rows, :], pre_ref[layer], preferred_element_type=jnp.float32)
        stage_enc[layer, place, :] = value.astype(jnp.bfloat16)
        pltpu.make_async_copy(stage_enc.at[layer, place], enc_out.at[layer, place], enc_sem).start()

    steps, enc_steps = tile // chunk, width // span
    writes = [(dec_step, index, step) for index in reversed(range(pairs)) for step in range(steps)]
    first = 2 * len(writes) // 3
    for step_of, *place in writes[:first]:
        step_of(*place)
    writes = writes[first:]
    for layer in reversed(range(layers)):
        share = -(-len(writes) // steps)
        for step in range(steps):
            pre_step(layer, step)
            if layer < layers - 1:
                for step_of, *place in writes[step * share : (step + 1) * share]:
                    step_of(*place)
        if layer < layers - 1:
            writes = []
        writes = writes + [(enc_step, layer, step) for step in range(enc_steps)]
    for step_of, *place in writes:
        step_of(*place)

    pltpu.make_async_copy(stage_dec, dec_out, dec_sem).wait()
    pltpu.make_async_copy(stage_enc, enc_out, enc_sem).wait()


def backward(scale, parts, feats, feats_t, x_t, dec_weight):
    layers, tokens, tile = feats.shape
    pairs, _, width = dec_weight.shape
    return pl.pallas_call(
        functools.partial(backward_kernel, scale),
        out_shape=(
            jax.ShapeDtypeStruct((layers, width, tile), jnp.bfloat16),
            jax.ShapeDtypeStruct((layers, tile), jnp.float32),
            jax.ShapeDtypeStruct((pairs, tile, width), jnp.bfloat16),
        ),
        in_specs=[WHOLE] * (len(parts) + 4),
        out_specs=[HELD, WHOLE, HELD],
        scratch_shapes=[
            pltpu.VMEM((tokens, layers * width), jnp.bfloat16),
            pltpu.VMEM((layers, tokens, tile), jnp.bfloat16),
            pltpu.VMEM((pairs, tile, width), jnp.bfloat16),
            pltpu.VMEM((layers, width, tile), jnp.bfloat16),
            pltpu.SemaphoreType.DMA,
            pltpu.SemaphoreType.DMA,
        ],
        compiler_params=params(28 * MIB),
        cost_estimate=cost(10 * tokens * dec_weight.size, 0),
        name="backward",
    )(*parts, feats, feats_t, x_t, in_vmem(dec_weight))


def local(store_inputs, store_targets, row_ids, enc_weight, enc_bias, dec_weight):
    size = lax.axis_size("feat")
    rows = row_ids.shape[0]
    scale = 1.0 / math.sqrt(rows * size)
    picked_in, picked_out = pick(row_ids, store_inputs, store_targets)
    parts, enc_near, dec_near = gather_rows(
        picked_in, size, load(enc_weight), functools.partial(load, dec_weight)
    )
    keep, send, feats, x = forward(parts, enc_near, enc_bias, dec_near)
    turned = turn(x, feats)
    own = scatter_sums(keep, send, size, rows)
    errors_own = (own - picked_out.astype(jnp.float32)).astype(jnp.bfloat16)
    parts, (x_t, feats_t), _ = gather_rows(errors_own, size, turned)
    return backward(scale, parts, feats, feats_t, x_t, dec_near)


def solution(mesh):
    in_specs = (
        P(None, ("group", "feat"), None),
        P(None, ("group", "feat"), None),
        P(("group", "feat")),
        P(None, None, "feat"),
        P(None, "feat"),
        P(None, "feat", None),
    )
    out_specs = (P("group", None, "feat"), P("group", "feat"), P("group", "feat", None))
    return jax.shard_map(local, mesh=mesh, in_specs=in_specs, out_specs=out_specs, check_vma=False)
```

```python
import functools
import math

import jax
import jax.numpy as jnp
from jax import lax
from jax.experimental import pallas as pl
from jax.experimental.pallas import tpu as pltpu
from jax.sharding import PartitionSpec as P


MIB = 1 << 20
WHOLE = pl.BlockSpec(memory_space=pltpu.VMEM)
HELD = pl.BlockSpec(memory_space=pl.ANY)


def pair_list(layers):
    return [(source, target) for source in range(layers) for target in range(source, layers)]


def params(limit):
    return pltpu.CompilerParams(vmem_limit_bytes=limit)


def cost(flops, moved):
    return pl.CostEstimate(flops=int(flops), transcendentals=0, bytes_accessed=int(moved))


def in_vmem(array):
    return pltpu.with_memory_space_constraint(array, pltpu.VMEM)


def swap(value, mask, size):
    return lax.ppermute(value, "feat", [(index, index ^ mask) for index in range(size)])


def gather_rows(own, size, beside=(), later=None):
    if size < 8:
        even = own if size == 2 else jnp.concatenate([own, swap(own, 2, size)], axis=0)
        return [even, swap(even, 1, size)], beside, later() if later else None
    far = [4 * step for step in range(1, size // 4)]
    got = {mask: swap(own, mask, size) for mask in far}
    side = swap(own, 2, size)
    late = [swap(got[far[0]], 2, size)]
    rest, beside = lax.optimization_barrier(([got[mask] for mask in far[1:]], beside))
    late.append(swap(jnp.concatenate(rest, axis=0), 2, size))
    early = jnp.concatenate([own, got[far[0]]] + rest + [side], axis=0)
    early_pair = swap(early, 1, size)
    late = jnp.concatenate(late, axis=0)
    made = None
    if later:
        late, made = lax.optimization_barrier((late, later(after=rest[:1])))
    return [early, late, early_pair, swap(late, 1, size)], beside, made


def scatter_sums(keep, send, size, rows, beside):
    got = swap(send, 1, size) if size > 1 else send
    pair = (keep.astype(jnp.float32) + got.astype(jnp.float32)).astype(jnp.bfloat16)
    count = max(size // 4, 1)

    def block(start, stop):
        return pair[start * rows : stop * rows]

    def total(left, right):
        return left.astype(jnp.float32) + right.astype(jnp.float32)

    own = block(0, 1).astype(jnp.float32)
    if size < 4:
        return own, beside
    if size < 8:
        return own + swap(block(1, 2), 2, size).astype(jnp.float32), beside
    outer = swap(block(count + 2, 2 * count), 2, size)
    inner = swap(block(count, count + 2), 2, size)
    outer, beside = lax.optimization_barrier((outer, beside))
    far = total(block(2, count), outer).astype(jnp.bfloat16)
    near = total(block(1, 2), inner[rows:]).astype(jnp.bfloat16)
    own = own + inner[:rows].astype(jnp.float32)
    sums = [
        swap(far[(slot - 2) * rows : (slot - 1) * rows], 4 * slot, size) for slot in reversed(range(2, count))
    ]
    sums.append(swap(near, 4, size))
    for value in sums:
        own = own + value.astype(jnp.float32)
    return own, beside


def pick_kernel(ids_hbm, in_hbm, out_hbm, picked_in, picked_out, ids_ref, in_ref, out_ref, sems):
    layers, buf, width = in_ref.shape
    rows = ids_ref.shape[0]
    copies = [
        pltpu.make_async_copy(ids_hbm, ids_ref, sems.at[0]),
        pltpu.make_async_copy(in_hbm, in_ref, sems.at[1]),
        pltpu.make_async_copy(out_hbm, out_ref, sems.at[2]),
    ]
    for copy in copies:
        copy.start()
    for copy in copies:
        copy.wait()
    place = lax.broadcasted_iota(jnp.int32, (rows, buf), 0)
    wanted = jnp.zeros((rows, buf), jnp.int32)
    for row in range(rows):
        wanted = jnp.where(place == row, ids_ref[row], wanted)
    hot = jnp.where(wanted == lax.broadcasted_iota(jnp.int32, (rows, buf), 1), 1.0, 0.0).astype(jnp.bfloat16)
    for layer in range(layers):
        columns = slice(layer * width, (layer + 1) * width)
        for ref, picked in ((in_ref, picked_in), (out_ref, picked_out)):
            picked[:, columns] = jnp.dot(hot, ref[layer], preferred_element_type=jnp.float32).astype(jnp.bfloat16)


def pick(row_ids, store_inputs, store_targets):
    layers, _, width = store_inputs.shape
    shape = jax.ShapeDtypeStruct((row_ids.shape[0], layers * width), jnp.bfloat16)
    return pl.pallas_call(
        pick_kernel,
        out_shape=(shape, shape),
        in_specs=[HELD] * 3,
        out_specs=[WHOLE, WHOLE],
        scratch_shapes=[
            pltpu.SMEM(row_ids.shape, jnp.int32),
            pltpu.VMEM(store_inputs.shape, jnp.bfloat16),
            pltpu.VMEM(store_targets.shape, jnp.bfloat16),
            pltpu.SemaphoreType.DMA((3,)),
        ],
        compiler_params=params(4 * MIB),
        name="pick",
    )(*(pltpu.with_memory_space_constraint(array, pltpu.HBM) for array in (row_ids, store_inputs, store_targets)))


def load_kernel(pieces, *refs):
    sources, outs, sems = refs[: len(pieces)], refs[-1 - len(pieces) : -1], refs[-1]
    copies = []
    for source, out, (first, count) in zip(sources, outs, pieces):
        for index in range(count):
            copies.append(
                pltpu.make_async_copy(source.at[first + index], out.at[index], sems.at[len(copies)])
            )
    for copy in copies:
        copy.start()
    for copy in copies:
        copy.wait()


def load(pieces, after=()):
    shapes = [(count,) + weight.shape[1:] for weight, _, count in pieces]
    moved = sum(4 * math.prod(shape) for shape in shapes)
    return pl.pallas_call(
        functools.partial(load_kernel, [(first, count) for _, first, count in pieces]),
        out_shape=[pltpu.VMEM(shape, jnp.bfloat16) for shape in shapes],
        in_specs=[HELD] * (len(pieces) + len(after)),
        out_specs=[WHOLE] * len(pieces),
        scratch_shapes=[pltpu.SemaphoreType.DMA((sum(count for _, _, count in pieces),))],
        compiler_params=params(2 * MIB),
        cost_estimate=cost(moved * 100, moved),
        name="load",
    )(*(pltpu.with_memory_space_constraint(weight, pltpu.HBM) for weight, _, _ in pieces), *after)


def join(part_refs, out_ref):
    start = 0
    for ref in part_refs:
        out_ref[start : start + ref.shape[0]] = ref[...]
        start += ref.shape[0]


def forward_kernel(*refs):
    parts, refs = refs[:-8], refs[-8:]
    enc_ref, bias_ref, dec_ref, last_ref, keep_ref, send_ref, feat_ref, x_ref = refs
    layers, width, tile = enc_ref.shape
    half = keep_ref.shape[0]
    held = dec_ref.shape[0]
    join(parts, x_ref)
    chunk = min(256, tile)
    for layer in range(layers):
        for step in range(tile // chunk):
            columns = pl.ds(step * chunk, chunk)
            value = jnp.dot(
                x_ref[:, layer * width : (layer + 1) * width],
                enc_ref[layer, :, columns],
                preferred_element_type=jnp.float32,
            )
            value = value + bias_ref[layer : layer + 1, columns]
            feat_ref[layer, :, columns] = jnp.maximum(value, 0.0).astype(jnp.bfloat16)

    span = min(512, width)
    for target in range(layers):
        wanted = [(index, source) for index, (source, goal) in enumerate(pair_list(layers)) if goal == target]
        for step in range(width // span):
            columns = pl.ds(step * span, span)
            total = None
            for index, source in wanted:
                weight = dec_ref[index, :, columns] if index < held else last_ref[index - held, :, columns]
                term = jnp.dot(feat_ref[source], weight, preferred_element_type=jnp.float32)
                total = term if total is None else total + term
            total = total.astype(jnp.bfloat16)
            places = pl.ds(target * width + step * span, span)
            keep_ref[:, places] = total[:half]
            send_ref[:, places] = total[half:]


def forward(parts, enc_weight, enc_bias, dec_near, dec_last):
    layers, _, tile = enc_weight.shape
    half, wide = sum(part.shape[0] for part in parts) // 2, parts[0].shape[1]
    side = jax.ShapeDtypeStruct((half, wide), jnp.bfloat16)
    return pl.pallas_call(
        forward_kernel,
        out_shape=(
            side,
            side,
            jax.ShapeDtypeStruct((layers, 2 * half, tile), jnp.bfloat16),
            jax.ShapeDtypeStruct((2 * half, wide), jnp.bfloat16),
        ),
        in_specs=[WHOLE] * (len(parts) + 4),
        out_specs=[WHOLE] * 4,
        compiler_params=params(12 * MIB),
        cost_estimate=cost(4 * half * (enc_weight.size + dec_near.size + dec_last.size), 0),
        name="forward",
    )(
        *parts,
        in_vmem(enc_weight),
        enc_bias,
        in_vmem(dec_near),
        in_vmem(dec_last),
    )


def turn_kernel(*refs):
    outs = iter(refs[len(refs) // 2 :])
    for ref in refs[: len(refs) // 2]:
        out = next(outs)
        if len(ref.shape) == 2:
            out[...] = ref[...].T
        else:
            for index in range(ref.shape[0]):
                out[index] = ref[index].T


def turn(arrays):
    shapes = [array.shape[:-2] + (array.shape[-1], array.shape[-2]) for array in arrays]
    return pl.pallas_call(
        turn_kernel,
        out_shape=[pltpu.VMEM(shape, jnp.bfloat16) for shape in shapes],
        in_specs=[WHOLE] * len(arrays),
        out_specs=[WHOLE] * len(arrays),
        compiler_params=params(8 * MIB),
        cost_estimate=cost(1000 * sum(array.size for array in arrays), 0),
        name="turn",
    )(*(in_vmem(array) for array in arrays))


def backward_kernel(scale, *refs):
    parts, refs = refs[:-14], refs[-14:]
    feat_ref, feat_t_ref, x_t_ref, near_t_ref, last_t_ref, enc_out, bias_out, dec_out = refs[:8]
    e_ref, pre_ref, stage_dec, stage_enc, dec_sem, enc_sem = refs[8:]
    pairs, tile, width = stage_dec.shape
    held = near_t_ref.shape[0]
    layers = feat_ref.shape[0]
    pair_of = pair_list(layers)
    join(parts, e_ref)
    chunk = min(256, tile)
    span = min(512, width)

    def dec_step(index, step):
        source, target = pair_of[index]
        place = pl.ds(step * chunk, chunk)
        value = jnp.dot(
            feat_t_ref[source, place, :],
            e_ref[:, target * width : (target + 1) * width],
            preferred_element_type=jnp.float32,
        )
        stage_dec[index, place, :] = (scale * value).astype(jnp.bfloat16)
        pltpu.make_async_copy(stage_dec.at[index, place], dec_out.at[index, place], dec_sem).start()

    def pre_step(layer, step):
        place = pl.ds(step * chunk, chunk)
        total = None
        for index, (source, target) in enumerate(pair_of):
            if source == layer:
                weight = near_t_ref[index, :, place] if index < held else last_t_ref[index - held, :, place]
                term = jnp.dot(
                    e_ref[:, target * width : (target + 1) * width], weight, preferred_element_type=jnp.float32
                )
                total = term if total is None else total + term
        pre = jnp.where(feat_ref[layer, :, place] > 0, total, 0.0) * scale
        bias_out[layer : layer + 1, place] = jnp.sum(pre, axis=0, keepdims=True)
        pre_ref[layer, :, place] = pre.astype(jnp.bfloat16)

    def enc_step(layer, step):
        place = pl.ds(step * span, span)
        rows = pl.ds(layer * width + step * span, span)
        value = jnp.dot(x_t_ref[rows, :], pre_ref[layer], preferred_element_type=jnp.float32)
        stage_enc[layer, place, :] = value.astype(jnp.bfloat16)
        pltpu.make_async_copy(stage_enc.at[layer, place], enc_out.at[layer, place], enc_sem).start()

    steps, enc_steps = tile // chunk, width // span
    writes = [(dec_step, index, step) for index in reversed(range(pairs)) for step in range(steps)]
    first = 2 * len(writes) // 3
    for step_of, *place in writes[:first]:
        step_of(*place)
    writes = writes[first:]
    for layer in reversed(range(layers)):
        share = -(-len(writes) // steps)
        for step in range(steps):
            pre_step(layer, step)
            if layer < layers - 1:
                for step_of, *place in writes[step * share : (step + 1) * share]:
                    step_of(*place)
        if layer < layers - 1:
            writes = []
        writes = writes + [(enc_step, layer, step) for step in range(enc_steps)]
    for step_of, *place in writes:
        step_of(*place)

    pltpu.make_async_copy(stage_dec, dec_out, dec_sem).wait()
    pltpu.make_async_copy(stage_enc, enc_out, enc_sem).wait()


def backward(scale, parts, feats, feats_t, x_t, near_t, last_t):
    layers, tokens, tile = feats.shape
    pairs, width = near_t.shape[0] + last_t.shape[0], near_t.shape[1]
    return pl.pallas_call(
        functools.partial(backward_kernel, scale),
        out_shape=(
            jax.ShapeDtypeStruct((layers, width, tile), jnp.bfloat16),
            jax.ShapeDtypeStruct((layers, tile), jnp.float32),
            jax.ShapeDtypeStruct((pairs, tile, width), jnp.bfloat16),
        ),
        in_specs=[WHOLE] * (len(parts) + 5),
        out_specs=[HELD, WHOLE, HELD],
        scratch_shapes=[
            pltpu.VMEM((tokens, layers * width), jnp.bfloat16),
            pltpu.VMEM((layers, tokens, tile), jnp.bfloat16),
            pltpu.VMEM((pairs, tile, width), jnp.bfloat16),
            pltpu.VMEM((layers, width, tile), jnp.bfloat16),
            pltpu.SemaphoreType.DMA,
            pltpu.SemaphoreType.DMA,
        ],
        compiler_params=params(28 * MIB),
        cost_estimate=cost(10 * tokens * pairs * tile * width, 0),
        name="backward",
    )(*parts, feats, *(in_vmem(array) for array in (feats_t, x_t, near_t, last_t)))


def local(store_inputs, store_targets, row_ids, enc_weight, enc_bias, dec_weight):
    size = lax.axis_size("feat")
    rows = row_ids.shape[0]
    scale = 1.0 / math.sqrt(rows * size)
    picked_in, picked_out = pick(row_ids, store_inputs, store_targets)
    held = dec_weight.shape[0] - 1
    parts, (enc_near, dec_last), (dec_near,) = gather_rows(
        picked_in,
        size,
        load([(enc_weight, 0, enc_weight.shape[0]), (dec_weight, held, 1)]),
        functools.partial(load, [(dec_weight, 0, held)]),
    )
    keep, send, feats, x = forward(parts, enc_near, enc_bias, dec_near, dec_last)
    flipped = turn([dec_near, dec_last])
    own, (near_t, last_t) = scatter_sums(keep, send, size, rows, flipped)
    errors_own = (own - picked_out.astype(jnp.float32)).astype(jnp.bfloat16)
    parts, (x_t, feats_t), _ = gather_rows(errors_own, size, turn([x, feats]))
    return backward(scale, parts, feats, feats_t, x_t, near_t, last_t)


def solution(mesh):
    in_specs = (
        P(None, ("group", "feat"), None),
        P(None, ("group", "feat"), None),
        P(("group", "feat")),
        P(None, None, "feat"),
        P(None, "feat"),
        P(None, "feat", None),
    )
    out_specs = (P("group", None, "feat"), P("group", "feat"), P("group", "feat", None))
    return jax.shard_map(local, mesh=mesh, in_specs=in_specs, out_specs=out_specs, check_vma=False)
```

```python
import functools
import math

import jax
import jax.numpy as jnp
from jax import lax
from jax.experimental import pallas as pl
from jax.experimental.pallas import tpu as pltpu
from jax.sharding import PartitionSpec as P


MIB = 1 << 20
WHOLE = pl.BlockSpec(memory_space=pltpu.VMEM)
HELD = pl.BlockSpec(memory_space=pl.ANY)


def pair_list(layers):
    return [(source, target) for source in range(layers) for target in range(source, layers)]


def params(limit):
    return pltpu.CompilerParams(vmem_limit_bytes=limit)


def cost(flops, moved):
    return pl.CostEstimate(flops=int(flops), transcendentals=0, bytes_accessed=int(moved))


def in_vmem(array):
    return pltpu.with_memory_space_constraint(array, pltpu.VMEM)


def swap(value, mask, size):
    return lax.ppermute(value, "feat", [(index, index ^ mask) for index in range(size)])


def gather_rows(own, size, beside=(), later=None):
    if size < 8:
        even = own if size == 2 else jnp.concatenate([own, swap(own, 2, size)], axis=0)
        return [even, swap(even, 1, size)], beside, later() if later else None
    far = [4 * step for step in range(1, size // 4)]
    got = {mask: swap(own, mask, size) for mask in far}
    side = swap(own, 2, size)
    late = [swap(got[far[0]], 2, size)]
    rest, beside = lax.optimization_barrier(([got[mask] for mask in far[1:]], beside))
    late.append(swap(jnp.concatenate(rest, axis=0), 2, size))
    early = jnp.concatenate([own, got[far[0]]] + rest + [side], axis=0)
    early_pair = swap(early, 1, size)
    late = jnp.concatenate(late, axis=0)
    made = None
    if later:
        late, made = lax.optimization_barrier((late, later(after=rest[:1])))
    return [early, late, early_pair, swap(late, 1, size)], beside, made


def scatter_sums(keep, send, size, rows, beside):
    got = swap(send, 1, size) if size > 1 else send
    pair = (keep.astype(jnp.float32) + got.astype(jnp.float32)).astype(jnp.bfloat16)
    count = max(size // 4, 1)

    def block(start, stop):
        return pair[start * rows : stop * rows]

    def total(left, right):
        return left.astype(jnp.float32) + right.astype(jnp.float32)

    own = block(0, 1).astype(jnp.float32)
    if size < 4:
        return own, beside
    if size < 8:
        return own + swap(block(1, 2), 2, size).astype(jnp.float32), beside
    outer = swap(block(count + 2, 2 * count), 2, size)
    inner = swap(block(count, count + 2), 2, size)
    outer, beside = lax.optimization_barrier((outer, beside))
    far = total(block(2, count), outer).astype(jnp.bfloat16)
    near = total(block(1, 2), inner[rows:]).astype(jnp.bfloat16)
    own = own + inner[:rows].astype(jnp.float32)
    sums = [swap(far[(slot - 2) * rows : (slot - 1) * rows], 4 * slot, size) for slot in range(2, count)]
    sums.append(swap(near, 4, size))
    for value in sums:
        own = own + value.astype(jnp.float32)
    return own, beside


def pick_kernel(ids_hbm, in_hbm, out_hbm, picked_in, picked_out, ids_ref, in_ref, out_ref, sems):
    layers, buf, width = in_ref.shape
    rows = ids_ref.shape[0]
    copies = [
        pltpu.make_async_copy(ids_hbm, ids_ref, sems.at[0]),
        pltpu.make_async_copy(in_hbm, in_ref, sems.at[1]),
        pltpu.make_async_copy(out_hbm, out_ref, sems.at[2]),
    ]
    for copy in copies:
        copy.start()
    for copy in copies:
        copy.wait()
    place = lax.broadcasted_iota(jnp.int32, (rows, buf), 0)
    wanted = jnp.zeros((rows, buf), jnp.int32)
    for row in range(rows):
        wanted = jnp.where(place == row, ids_ref[row], wanted)
    hot = jnp.where(wanted == lax.broadcasted_iota(jnp.int32, (rows, buf), 1), 1.0, 0.0).astype(jnp.bfloat16)
    for layer in range(layers):
        columns = slice(layer * width, (layer + 1) * width)
        for ref, picked in ((in_ref, picked_in), (out_ref, picked_out)):
            picked[:, columns] = jnp.dot(hot, ref[layer], preferred_element_type=jnp.float32).astype(jnp.bfloat16)


def pick(row_ids, store_inputs, store_targets):
    layers, _, width = store_inputs.shape
    shape = jax.ShapeDtypeStruct((row_ids.shape[0], layers * width), jnp.bfloat16)
    return pl.pallas_call(
        pick_kernel,
        out_shape=(shape, shape),
        in_specs=[HELD] * 3,
        out_specs=[WHOLE, WHOLE],
        scratch_shapes=[
            pltpu.SMEM(row_ids.shape, jnp.int32),
            pltpu.VMEM(store_inputs.shape, jnp.bfloat16),
            pltpu.VMEM(store_targets.shape, jnp.bfloat16),
            pltpu.SemaphoreType.DMA((3,)),
        ],
        compiler_params=params(4 * MIB),
        name="pick",
    )(*(pltpu.with_memory_space_constraint(array, pltpu.HBM) for array in (row_ids, store_inputs, store_targets)))


def load_kernel(pieces, *refs):
    sources, outs, sems = refs[: len(pieces)], refs[-1 - len(pieces) : -1], refs[-1]
    copies = []
    for source, out, (first, count) in zip(sources, outs, pieces):
        for index in range(count):
            copies.append(
                pltpu.make_async_copy(source.at[first + index], out.at[index], sems.at[len(copies)])
            )
    for copy in copies:
        copy.start()
    for copy in copies:
        copy.wait()


def load(pieces, after=()):
    shapes = [(count,) + weight.shape[1:] for weight, _, count in pieces]
    moved = sum(4 * math.prod(shape) for shape in shapes)
    return pl.pallas_call(
        functools.partial(load_kernel, [(first, count) for _, first, count in pieces]),
        out_shape=[pltpu.VMEM(shape, jnp.bfloat16) for shape in shapes],
        in_specs=[HELD] * (len(pieces) + len(after)),
        out_specs=[WHOLE] * len(pieces),
        scratch_shapes=[pltpu.SemaphoreType.DMA((sum(count for _, _, count in pieces),))],
        compiler_params=params(2 * MIB),
        cost_estimate=cost(moved * 100, moved),
        name="load",
    )(*(pltpu.with_memory_space_constraint(weight, pltpu.HBM) for weight, _, _ in pieces), *after)


def join(part_refs, out_ref):
    start = 0
    for ref in part_refs:
        out_ref[start : start + ref.shape[0]] = ref[...]
        start += ref.shape[0]


def forward_kernel(*refs):
    parts, refs = refs[:-8], refs[-8:]
    enc_ref, bias_ref, dec_ref, last_ref, keep_ref, send_ref, feat_ref, x_ref = refs
    layers, width, tile = enc_ref.shape
    half = keep_ref.shape[0]
    held = dec_ref.shape[0]
    join(parts, x_ref)
    chunk = min(256, tile)
    for layer in range(layers):
        for step in range(tile // chunk):
            columns = pl.ds(step * chunk, chunk)
            value = jnp.dot(
                x_ref[:, layer * width : (layer + 1) * width],
                enc_ref[layer, :, columns],
                preferred_element_type=jnp.float32,
            )
            value = value + bias_ref[layer : layer + 1, columns]
            feat_ref[layer, :, columns] = jnp.maximum(value, 0.0).astype(jnp.bfloat16)

    span = min(512, width)
    for target in range(layers):
        wanted = [(index, source) for index, (source, goal) in enumerate(pair_list(layers)) if goal == target]
        for step in range(width // span):
            columns = pl.ds(step * span, span)
            total = None
            for index, source in wanted:
                weight = dec_ref[index, :, columns] if index < held else last_ref[index - held, :, columns]
                term = jnp.dot(feat_ref[source], weight, preferred_element_type=jnp.float32)
                total = term if total is None else total + term
            total = total.astype(jnp.bfloat16)
            places = pl.ds(target * width + step * span, span)
            keep_ref[:, places] = total[:half]
            send_ref[:, places] = total[half:]


def forward(parts, enc_weight, enc_bias, dec_near, dec_last):
    layers, _, tile = enc_weight.shape
    half, wide = sum(part.shape[0] for part in parts) // 2, parts[0].shape[1]
    side = jax.ShapeDtypeStruct((half, wide), jnp.bfloat16)
    return pl.pallas_call(
        forward_kernel,
        out_shape=(
            side,
            side,
            jax.ShapeDtypeStruct((layers, 2 * half, tile), jnp.bfloat16),
            jax.ShapeDtypeStruct((2 * half, wide), jnp.bfloat16),
        ),
        in_specs=[WHOLE] * (len(parts) + 4),
        out_specs=[WHOLE] * 4,
        compiler_params=params(12 * MIB),
        cost_estimate=cost(4 * half * (enc_weight.size + dec_near.size + dec_last.size), 0),
        name="forward",
    )(
        *parts,
        in_vmem(enc_weight),
        enc_bias,
        in_vmem(dec_near),
        in_vmem(dec_last),
    )


def turn_kernel(*refs):
    outs = iter(refs[len(refs) // 2 :])
    for ref in refs[: len(refs) // 2]:
        out = next(outs)
        if len(ref.shape) == 2:
            out[...] = ref[...].T
        else:
            for index in range(ref.shape[0]):
                out[index] = ref[index].T


def turn(arrays):
    shapes = [array.shape[:-2] + (array.shape[-1], array.shape[-2]) for array in arrays]
    return pl.pallas_call(
        turn_kernel,
        out_shape=[pltpu.VMEM(shape, jnp.bfloat16) for shape in shapes],
        in_specs=[WHOLE] * len(arrays),
        out_specs=[WHOLE] * len(arrays),
        compiler_params=params(8 * MIB),
        cost_estimate=cost(1000 * sum(array.size for array in arrays), 0),
        name="turn",
    )(*(in_vmem(array) for array in arrays))


def backward_kernel(scale, *refs):
    parts, refs = refs[:-14], refs[-14:]
    feat_ref, feat_t_ref, x_t_ref, near_t_ref, last_t_ref, enc_out, bias_out, dec_out = refs[:8]
    e_ref, pre_ref, stage_dec, stage_enc, dec_sem, enc_sem = refs[8:]
    pairs, tile, width = stage_dec.shape
    held = near_t_ref.shape[0]
    layers = feat_ref.shape[0]
    pair_of = pair_list(layers)
    join(parts, e_ref)
    chunk = min(256, tile)
    span = min(512, width)

    def dec_step(index, step):
        source, target = pair_of[index]
        place = pl.ds(step * chunk, chunk)
        value = jnp.dot(
            feat_t_ref[source, place, :],
            e_ref[:, target * width : (target + 1) * width],
            preferred_element_type=jnp.float32,
        )
        stage_dec[index, place, :] = (scale * value).astype(jnp.bfloat16)
        pltpu.make_async_copy(stage_dec.at[index, place], dec_out.at[index, place], dec_sem).start()

    def pre_step(layer, step):
        place = pl.ds(step * chunk, chunk)
        total = None
        for index, (source, target) in enumerate(pair_of):
            if source == layer:
                weight = near_t_ref[index, :, place] if index < held else last_t_ref[index - held, :, place]
                term = jnp.dot(
                    e_ref[:, target * width : (target + 1) * width], weight, preferred_element_type=jnp.float32
                )
                total = term if total is None else total + term
        pre = jnp.where(feat_ref[layer, :, place] > 0, total, 0.0) * scale
        bias_out[layer : layer + 1, place] = jnp.sum(pre, axis=0, keepdims=True)
        pre_ref[layer, :, place] = pre.astype(jnp.bfloat16)

    def enc_step(layer, step):
        place = pl.ds(step * span, span)
        rows = pl.ds(layer * width + step * span, span)
        value = jnp.dot(x_t_ref[rows, :], pre_ref[layer], preferred_element_type=jnp.float32)
        stage_enc[layer, place, :] = value.astype(jnp.bfloat16)
        pltpu.make_async_copy(stage_enc.at[layer, place], enc_out.at[layer, place], enc_sem).start()

    steps, enc_steps = tile // chunk, width // span
    writes = [(dec_step, index, step) for index in reversed(range(pairs)) for step in range(steps)]
    first = 2 * len(writes) // 3
    for step_of, *place in writes[:first]:
        step_of(*place)
    writes = writes[first:]
    for layer in reversed(range(layers)):
        share = -(-len(writes) // steps)
        for step in range(steps):
            pre_step(layer, step)
            if layer < layers - 1:
                for step_of, *place in writes[step * share : (step + 1) * share]:
                    step_of(*place)
        if layer < layers - 1:
            writes = []
        writes = writes + [(enc_step, layer, step) for step in range(enc_steps)]
    for step_of, *place in writes:
        step_of(*place)

    pltpu.make_async_copy(stage_dec, dec_out, dec_sem).wait()
    pltpu.make_async_copy(stage_enc, enc_out, enc_sem).wait()


def backward(scale, parts, feats, feats_t, x_t, near_t, last_t):
    layers, tokens, tile = feats.shape
    pairs, width = near_t.shape[0] + last_t.shape[0], near_t.shape[1]
    return pl.pallas_call(
        functools.partial(backward_kernel, scale),
        out_shape=(
            jax.ShapeDtypeStruct((layers, width, tile), jnp.bfloat16),
            jax.ShapeDtypeStruct((layers, tile), jnp.float32),
            jax.ShapeDtypeStruct((pairs, tile, width), jnp.bfloat16),
        ),
        in_specs=[WHOLE] * (len(parts) + 5),
        out_specs=[HELD, WHOLE, HELD],
        scratch_shapes=[
            pltpu.VMEM((tokens, layers * width), jnp.bfloat16),
            pltpu.VMEM((layers, tokens, tile), jnp.bfloat16),
            pltpu.VMEM((pairs, tile, width), jnp.bfloat16),
            pltpu.VMEM((layers, width, tile), jnp.bfloat16),
            pltpu.SemaphoreType.DMA,
            pltpu.SemaphoreType.DMA,
        ],
        compiler_params=params(24 * MIB),
        cost_estimate=cost(10 * tokens * pairs * tile * width, 0),
        name="backward",
    )(*parts, feats, *(in_vmem(array) for array in (feats_t, x_t, near_t, last_t)))


def local(store_inputs, store_targets, row_ids, enc_weight, enc_bias, dec_weight):
    size = lax.axis_size("feat")
    rows = row_ids.shape[0]
    scale = 1.0 / math.sqrt(rows * size)
    picked_in, picked_out = pick(row_ids, store_inputs, store_targets)
    held = dec_weight.shape[0] - 1
    parts, (enc_near,), (dec_last, dec_near) = gather_rows(
        picked_in,
        size,
        load([(enc_weight, 0, enc_weight.shape[0])]),
        functools.partial(load, [(dec_weight, held, 1), (dec_weight, 0, held)]),
    )
    keep, send, feats, x = forward(parts, enc_near, enc_bias, dec_near, dec_last)
    flipped = turn([dec_near, dec_last])
    own, (near_t, last_t) = scatter_sums(keep, send, size, rows, flipped)
    errors_own = (own - picked_out.astype(jnp.float32)).astype(jnp.bfloat16)
    parts, (x_t, feats_t), _ = gather_rows(errors_own, size, turn([x, feats]))
    return backward(scale, parts, feats, feats_t, x_t, near_t, last_t)


def solution(mesh):
    in_specs = (
        P(None, ("group", "feat"), None),
        P(None, ("group", "feat"), None),
        P(("group", "feat")),
        P(None, None, "feat"),
        P(None, "feat"),
        P(None, "feat", None),
    )
    out_specs = (P("group", None, "feat"), P("group", "feat"), P("group", "feat", None))
    return jax.shard_map(local, mesh=mesh, in_specs=in_specs, out_specs=out_specs, check_vma=False)
```
